32 devices in a mesh: runs: 2 (over x), brick: 16 (over z, y, core).
Axes of the slice: x: 2, y: 2, z: 4, core: 2. Of those that a mesh axis runs over, the one named last changes fastest.
Arguments:
- grid: float32 [3, 8388608], P(None, ('runs', 'brick')), parts along dimension 1, may hold values from 0.2 to 4
- distribution: float32 [64, 16384], P(None, ('runs', 'brick')), parts along dimension 1, may hold values from 0.02 to 1
- owner_ids: int32 [16384, 1], P(('runs', 'brick')), parts along dimension 0, may hold values from 0 to 15; in each aligned block of 512 rows (0 to 511, 512 to 1023, ...) at most 64 rows name the same one
- coords: int32 [3, 16384], P(None, ('runs', 'brick')), parts along dimension 1, may hold values from 0 to 62
- fracs: float32 [3, 16384], P(None, ('runs', 'brick')), parts along dimension 1, may hold values from 0 to 1
- counts: int32 [16384], P(('runs', 'brick')), parts along dimension 0, may hold values from 1 to 4
- kernel: float32 [64, 64], replicated, may hold values from 0.002 to 0.2
- redist: float32 [64, 64], replicated, may hold values from 0.001 to 0.05
- shatter: float32 [64, 64], replicated, may hold values from 0.001 to 0.05
Outputs:
- updated: float32 [64, 16384], P(None, ('runs', 'brick')), parts along dimension 1
The draws below stay inside these ranges and needn't reach their ends.
There are 2 independent parts, one for each index of `runs`. The reference program is written for one: setup_inputs(seed, part) draws one part's arguments, and reference() takes and returns one part's arrays. A program takes and returns all parts, laid end to end along the dimension named above; an argument that names none is the same for every part. Nothing has to cross between parts.
Inputs may be any that keep to these rules, and one draw needn't show every extreme that they name: `owner_ids`: in the rows of one device at most 64 tracers name one brick, a bound that some block reaches of them.
All inputs are finite; a program needn't handle non-finite values.
Results may differ from the reference program's by a relative error of at most 0.0001.
Values sent between devices are 32-bit elements; how exact they have to be, the bound alone decides.
No kernel may reach another device: no remote copies, remote signals or barrier semaphores. Data moves between devices by JAX's collectives and lax.ppermute only.
A program may use at most 256 MiB of HBM per device.

```python
import math
import jax
import jax.numpy as jnp
import numpy as np
from jax import lax

BINS = 64
BS = 64
TR_DEV = 512
CAP = 64
CELLS = 262144
TRACERS = 8192
N_BRICK = 16


def touch_ends(entries, key, smallest, top_value):
    place = [jax.random.randint(jax.random.fold_in(key, axis), (), 0, length) for axis, length in enumerate(entries.shape)]
    main_axis = entries.shape.index(max(entries.shape))
    neighbour = place[:main_axis] + [(place[main_axis] + 1) % entries.shape[main_axis]] + place[main_axis + 1:]
    return entries.at[tuple(place)].set(smallest).at[tuple(neighbour)].set(top_value)


def levels(stream_key, extent, split, least, top_value):
    factor_of = 1.0
    for position, shards_of in split:
        draws = jax.random.uniform(jax.random.fold_in(jax.random.fold_in(stream_key, 6), position), (shards_of,), jnp.float32, least / len(split), top_value / len(split))
        factor_of = factor_of * jnp.repeat(jnp.exp(draws), extent[position] // shards_of).reshape((-1,) + (1,) * (len(extent) - 1 - position))
    return factor_of


def shared_out(key, own, number, rows, amount, top, most, skew):
    order = jax.random.permutation(key, amount)
    heavy_load, usual = shares(amount, rows * top, most, skew, True), shares(amount, rows * top, most, skew, False)
    places = jnp.arange(amount)

    def named(lengths, rotation):
        used = int((lengths > 0).sum())
        fixed = max(1, used // 4)
        passed = fixed + (places - fixed + rotation * (used - fixed)) % max(1, amount - fixed)
        return jnp.zeros((amount,), jnp.int32).at[order[jnp.where(places < fixed, places, passed)]].set(jnp.asarray(lengths, jnp.int32))

    lengths = jnp.where(number % 4 == 0, named(heavy_load, number // 4), named(usual, number - number // 4 - 1))
    mixed = jax.random.permutation(jax.random.fold_in(own, 3), amount)
    giver, sink = mixed[0:amount // 2 * 2:2], mixed[1:amount // 2 * 2:2]
    margin = jnp.minimum(lengths[giver] - 1, most - lengths[sink]) // 2
    margin = jnp.where((giver == order[0]) | (sink == order[0]) | (lengths[sink] == 0), 0, jnp.maximum(margin, 0))
    passed = jax.random.randint(jax.random.fold_in(own, 4), (amount // 2,), 0, 1 << 20) % (margin + 1)
    lengths = lengths.at[giver].add(-passed).at[sink].add(passed)
    items = jnp.searchsorted(jnp.cumsum(lengths), jnp.arange(rows * top), side="right").astype(jnp.int32)
    table = items.reshape(top, rows).T
    table = table[jax.random.permutation(jax.random.fold_in(own, 1), rows)]
    rotation = jax.random.randint(jax.random.fold_in(own, 2), (rows, 1), 0, top)
    return jnp.take_along_axis(table, (jnp.arange(top)[None, :] + rotation) % top, axis=1)


def shares(count, total, reach, skew, full):
    portions = [(1 << 20) // math.isqrt(rank ** skew) + 1 for rank in range(1, count + 1)]
    largest = reach if full else min(reach, max(-(-total // count), total * portions[0] // sum(portions)))
    least = 1 if total - largest >= count - 1 else 0
    holding, surplus = [largest] + [least] * (count - 1), total - largest - least * (count - 1)
    while surplus > 0:
        candidates = [i for i in range(1, count) if holding[i] < largest] or [i for i in range(1, count) if holding[i] < reach]
        mass, left = sum([portions[i] for i in candidates]), surplus
        for i in candidates:
            more = min(reach - holding[i], max(1, left * portions[i] // mass), surplus)
            holding[i] = holding[i] + more
            surplus = surplus - more
    return np.array(holding)


def setup_inputs(seed: int = 0, part: int = 0) -> dict:
    seeds = jax.random.split(jax.random.key(seed), 10)
    part_keys = jax.random.split(jax.random.fold_in(seeds[9], part), 10)
    grid = jnp.clip(jnp.exp(math.log(4.0) - 2.9957323 * jax.random.uniform(part_keys[0], (3, CELLS * N_BRICK), jnp.float32) ** levels(part_keys[0], (3, CELLS * N_BRICK), ((1, 16),), -0.2, 0.2)), 0.2, 4.0)
    distribution = jnp.clip(jnp.exp(math.log(1.0) - 3.912023 * jax.random.uniform(part_keys[1], (BINS, TRACERS), jnp.float32) ** levels(part_keys[1], (BINS, TRACERS), ((1, 16),), -0.2, 0.2)), 0.02, 1.0)
    owner_ids_keys = jax.random.split(jax.random.fold_in(part_keys[2], 1), TRACERS // TR_DEV)
    owner_ids_turns = jax.random.permutation(jax.random.fold_in(part_keys[2], 3), TRACERS // TR_DEV)
    owner_ids = jax.vmap(lambda own, number: shared_out(jax.random.fold_in(part_keys[2], 2), own, number, TR_DEV, N_BRICK, 1, CAP, 2))(owner_ids_keys, owner_ids_turns).reshape((TRACERS, 1))
    coords = touch_ends(jax.random.randint(part_keys[3], (3, TRACERS), 0, BS - 1), jax.random.fold_in(part_keys[3], 1), 0, (BS - 1) - 1).astype(jnp.int32)
    fracs = jnp.clip(1.0 * jax.random.uniform(part_keys[4], (3, TRACERS), jnp.float32) ** levels(part_keys[4], (3, TRACERS), ((1, 16),), -0.2, 0.2), 0.0, 1.0)
    counts = touch_ends(jax.random.randint(part_keys[5], (TRACERS,), 1, 5), jax.random.fold_in(part_keys[5], 1), 1, 4).astype(jnp.int32)
    kernel = jnp.clip(jnp.exp(jax.random.uniform(seeds[6], (BINS, BINS), jnp.float32, math.log(0.002), math.log(0.2))), 0.002, 0.2)
    redist = jnp.clip(jnp.exp(jax.random.uniform(seeds[7], (BINS, BINS), jnp.float32, math.log(0.001), math.log(0.05))), 0.001, 0.05)
    shatter = jnp.clip(jnp.exp(jax.random.uniform(seeds[8], (BINS, BINS), jnp.float32, math.log(0.001), math.log(0.05))), 0.001, 0.05)
    return dict(grid=grid, distribution=distribution, owner_ids=owner_ids, coords=coords, fracs=fracs, counts=counts, kernel=kernel, redist=redist, shatter=shatter)


def corner_sum(fields, coords, fracs, side, offset):
    total = jnp.zeros(fracs.shape, jnp.float32)
    for corner in range(8):
        first = corner // 4
        second = corner // 2 % 2
        third = corner % 2
        weight = jnp.ones(fracs.shape[1:], jnp.float32)
        weight = weight * (fracs[0] if first else 1.0 - fracs[0])
        weight = weight * (fracs[1] if second else 1.0 - fracs[1])
        weight = weight * (fracs[2] if third else 1.0 - fracs[2])
        where = ((coords[0] + first) * side + coords[1] + second) * side + coords[2] + third + offset
        picked = jnp.take(fields, where.astype(jnp.int32), axis=1)
        total = total + weight[None] * picked
    return total

def advance(dist, coag, shat, steps, kernel, redist, shatter):
    step_size = 1.0 / jnp.maximum(steps, 1).astype(jnp.float32)
    for section in range(4):
        kernel_dot = jnp.einsum('ij,j...->i...', kernel, dist, precision=lax.Precision.HIGHEST)
        collided = dist * kernel_dot
        gain = coag * jnp.einsum('ij,j...->i...', redist, collided, precision=lax.Precision.HIGHEST)
        gain = gain + shat * jnp.einsum('ij,j...->i...', shatter, dist, precision=lax.Precision.HIGHEST)
        loss = coag * kernel_dot + shat
        fresh = (dist + step_size * gain) / (1.0 + step_size * loss)
        dist = jnp.where(steps >= section + 1, fresh, dist)
    return dist

def reference(grid, distribution, owner_ids, coords, fracs, counts, kernel, redist, shatter):
    owner = owner_ids[:, 0]
    sampled = corner_sum(grid, coords, fracs, BS, owner * (BS * BS * BS))
    coag = sampled[0] * jnp.sqrt(sampled[1])
    shat = sampled[2] * sampled[1]
    return advance(distribution, coag, shat, counts, kernel, redist, shatter)
```

```python
import functools

import jax
import jax.numpy as jnp
from jax import lax
from jax.experimental import pallas as pl
from jax.experimental.pallas import tpu as pltpu
from jax.sharding import PartitionSpec as P

BS = 64
LANES = 128
ROWS_PER_TILE = LANES // BS
PLANE = BS * BS // LANES
NT = (((1,), (1,)), ((), ()))


def split3(x):
    hi = x.astype(jnp.bfloat16)
    rest = x - hi.astype(jnp.float32)
    mid = rest.astype(jnp.bfloat16)
    low = (rest - mid.astype(jnp.float32)).astype(jnp.bfloat16)
    return hi.astype(jnp.float32), mid.astype(jnp.float32), low.astype(jnp.float32)


def pack_kernel(bricks, capacity, owner_ref, coords_ref, fracs_ref, request_ref, rank_ref):
    tracers = owner_ref.shape[1]
    groups = tracers // LANES
    owner = owner_ref[...]
    brick = lax.broadcasted_iota(jnp.int32, (bricks, LANES), 0)
    row = lax.broadcasted_iota(jnp.int32, (LANES, 2 * LANES), 0)
    column = lax.broadcasted_iota(jnp.int32, (LANES, 2 * LANES), 1)
    before = jnp.where((row < column) | (column >= LANES), 1.0, 0.0).astype(jnp.bfloat16)
    member = [
        jnp.where(owner[:, g * LANES : (g + 1) * LANES] == brick, 1.0, 0.0) for g in range(groups)
    ]
    counted = jnp.dot(
        jnp.concatenate(member, axis=0).astype(jnp.bfloat16),
        before,
        preferred_element_type=jnp.float32,
    )
    base = jnp.zeros((bricks, LANES), jnp.float32)
    ranks = []
    for g in range(groups):
        block = counted[g * bricks : (g + 1) * bricks]
        ranks.append(jnp.sum(member[g] * (block[:, :LANES] + base), axis=0, keepdims=True))
        base = base + block[:, LANES:]
    rank = jnp.concatenate(ranks, axis=1)
    rank_ref[...] = rank.astype(jnp.int32)
    place = lax.broadcasted_iota(jnp.int32, (LANES, tracers), 0) % capacity
    onehot = jnp.where(rank == place.astype(jnp.float32), 1.0, 0.0).astype(jnp.bfloat16)
    coords = coords_ref[...].astype(jnp.float32)
    hi, mid, low = split3(fracs_ref[...])
    one = jnp.ones((1, tracers), jnp.float32)
    none = jnp.zeros((4, tracers), jnp.float32)
    parts = (
        jnp.concatenate([coords, one, hi, 0.0 * one], axis=0),
        jnp.concatenate([none, mid, 0.0 * one], axis=0),
        jnp.concatenate([none, low, 0.0 * one], axis=0),
    )
    total = None
    for part in parts:
        masked = jnp.concatenate(
            [jnp.where(owner == b, part, 0.0) for b in range(bricks)], axis=0
        ).astype(jnp.bfloat16)
        term = lax.dot_general(masked, onehot, NT, preferred_element_type=jnp.float32)
        total = term if total is None else total + term
    request_ref[...] = total.reshape(bricks, 8, LANES)


def sample_kernel(
    bricks, capacity, request_ref, grid_ref, reply_ref, staged, where_ref, frac_ref, lines, sem
):
    blocks = 4 * capacity // LANES
    first = request_ref[:, 0, :].astype(jnp.int32)
    second = request_ref[:, 1, :].astype(jnp.int32)
    shift = ROWS_PER_TILE.bit_length() - 1
    staged[0] = first * PLANE + (second >> shift)
    staged[1] = first * PLANE + ((second + 1) >> shift)
    valid = jnp.sum(request_ref[:, 3, :], axis=1, keepdims=True) * (capacity / LANES)
    staged[2] = jnp.broadcast_to(valid.astype(jnp.int32), (bricks, LANES))
    copies = [
        pltpu.make_async_copy(staged, where_ref, sem.at[0]),
        pltpu.make_async_copy(request_ref.at[:, 4, :], frac_ref, sem.at[1]),
    ]
    for copy in copies:
        copy.start()
    lane = lax.broadcasted_iota(jnp.int32, (3, LANES), 1)
    left = lane < BS
    for copy in copies:
        copy.wait()
    unroll = 8

    def gather(p, carry):
        count = where_ref[2, p, 0]

        def step(c, carry):
            for u in range(unroll):
                r = c * unroll + u
                upper = where_ref[0, p, r]
                lower = where_ref[1, p, r]
                f0 = frac_ref[p, r]
                near = jnp.where(left, grid_ref[lower], grid_ref[upper])
                far = jnp.where(left, grid_ref[lower + PLANE], grid_ref[upper + PLANE])
                line = near + f0 * (far - near)
                lines[pl.ds(p * (4 * capacity) + r, 3, stride=capacity), :] = line
            return carry

        return lax.fori_loop(0, (count + unroll - 1) // unroll, step, carry)

    lax.fori_loop(0, bricks, gather, 0)
    cell = lax.broadcasted_iota(jnp.int32, (BS, LANES), 0)

    def weigh(p):
        asked = request_ref[p]
        second = asked[1:2].astype(jnp.int32)
        third = asked[2:3].astype(jnp.int32)
        f1 = asked[5:6]
        f2 = asked[6:7]
        along = jnp.where(cell == third, 1.0 - f2, jnp.where(cell == third + 1, f2, 0.0))
        even = (second & 1) == 0
        top = jnp.where(even, 1.0 - f1, f1)
        bottom = jnp.where(even, f1, 1.0 - f1)
        rows = []
        for q in range(blocks):
            start = p * (4 * capacity) + q * LANES
            turned = lines[pl.ds(start, LANES), :].T
            crossed = turned[:BS] * top + turned[BS:] * bottom
            rows.append(jnp.sum(crossed * along, axis=0, keepdims=True))
        reply_ref[p] = jnp.concatenate(rows, axis=0)

    for p in range(bricks):
        weigh(p)


def advance_kernel(
    bricks,
    capacity,
    reply_ref,
    owner_ref,
    rank_ref,
    counts_ref,
    dist_ref,
    kernel_ref,
    redist_ref,
    shatter_ref,
    out_ref,
):
    tracers = owner_ref.shape[1]
    groups = tracers // LANES
    brick = lax.broadcasted_iota(jnp.int32, (bricks, LANES), 0)
    rows = [reply_ref[:, q, :] for q in range(reply_ref.shape[1])]
    fields = [[], [], []]
    for g in range(groups):
        lanes = slice(g * LANES, (g + 1) * LANES)
        mine = owner_ref[:, lanes] == brick
        rank = jnp.broadcast_to(rank_ref[:, lanes], (bricks, LANES))
        for f in range(3):
            q, offset = divmod(f * capacity, LANES)
            found = jnp.take_along_axis(rows[q], rank + offset, axis=1)
            fields[f].append(jnp.sum(jnp.where(mine, found, 0.0), axis=0, keepdims=True))
    density, temperature, metals = [jnp.concatenate(f, axis=1) for f in fields]
    coag = density * jnp.sqrt(temperature)
    shat = metals * temperature
    counts = counts_ref[...]
    h = 1.0 / jnp.maximum(counts, 1).astype(jnp.float32)

    def halves(x):
        hi = x.astype(jnp.bfloat16)
        return hi, (x - hi.astype(jnp.float32)).astype(jnp.bfloat16)

    def wide(x):
        hi, low = halves(x)
        return jnp.concatenate([hi, hi, low], axis=1)

    def tall(x):
        hi, low = halves(x)
        return jnp.concatenate([hi, low, hi], axis=0)

    def product(a, x):
        return jnp.dot(a, tall(x), preferred_element_type=jnp.float32)

    bins = dist_ref.shape[0]
    both = wide(jnp.concatenate([kernel_ref[...], shatter_ref[...]], axis=0))
    redist = wide(redist_ref[...])
    hcoag = h * coag
    hshat = h * shat
    n = dist_ref[...]
    for section in range(4):
        pair = product(both, n)
        kn = pair[:bins]
        broken = pair[bins:]
        moved = product(redist, n * kn)
        fresh = (n + (hcoag * moved + hshat * broken)) / (1.0 + (hcoag * kn + hshat))
        n = fresh if section == 0 else jnp.where(counts >= section + 1, fresh, n)
    out_ref[...] = n


def whole(*shape):
    return pl.BlockSpec(memory_space=pltpu.VMEM)


def shards(grid, distribution, owner_ids, coords, fracs, counts, kernel, redist, shatter):
    bricks = lax.axis_size("brick")
    tracers = distribution.shape[1]
    capacity = 2 * tracers // bricks
    blocks = 4 * capacity // LANES
    owner = owner_ids.reshape(1, tracers)
    vmem = pl.BlockSpec(memory_space=pltpu.VMEM)
    request, rank = pl.pallas_call(
        functools.partial(pack_kernel, bricks, capacity),
        out_shape=(
            jax.ShapeDtypeStruct((bricks, 8, LANES), jnp.float32),
            jax.ShapeDtypeStruct((1, tracers), jnp.int32),
        ),
        in_specs=[vmem] * 3,
        out_specs=(vmem, vmem),
        name="pack",
    )(owner, coords, fracs)
    asked = lax.all_to_all(request, "brick", split_axis=0, concat_axis=0, tiled=True)
    cells = grid.shape[1]
    tiles = grid.reshape(3, cells // LANES, LANES).transpose(1, 0, 2)
    reply = pl.pallas_call(
        functools.partial(sample_kernel, bricks, capacity),
        out_shape=jax.ShapeDtypeStruct((bricks, blocks, LANES), jnp.float32),
        in_specs=[vmem] * 2,
        out_specs=vmem,
        scratch_shapes=[
            pltpu.VMEM((3, bricks, LANES), jnp.int32),
            pltpu.SMEM((3, bricks, LANES), jnp.int32),
            pltpu.SMEM((bricks, LANES), jnp.float32),
            pltpu.VMEM((bricks * 4 * capacity, LANES), jnp.float32),
            pltpu.SemaphoreType.DMA((2,)),
        ],
        name="sample",
    )(asked, tiles)
    back = lax.all_to_all(reply, "brick", split_axis=0, concat_axis=0, tiled=True)
    return pl.pallas_call(
        functools.partial(advance_kernel, bricks, capacity),
        out_shape=jax.ShapeDtypeStruct(distribution.shape, jnp.float32),
        in_specs=[vmem] * 8,
        out_specs=vmem,
        name="advance",
    )(back, owner, rank, counts.reshape(1, tracers), distribution, kernel, redist, shatter)


def solution(mesh):
    in_specs = (
        P(None, ("runs", "brick")),
        P(None, ("runs", "brick")),
        P(("runs", "brick"), None),
        P(None, ("runs", "brick")),
        P(None, ("runs", "brick")),
        P(("runs", "brick")),
        P(),
        P(),
        P(),
    )
    out_specs = P(None, ("runs", "brick"))
    return jax.shard_map(shards, mesh=mesh, in_specs=in_specs, out_specs=out_specs, check_vma=False)
```

```python
import functools

import jax
import jax.numpy as jnp
from jax import lax
from jax.experimental import pallas as pl
from jax.experimental.pallas import tpu as pltpu
from jax.sharding import PartitionSpec as P

BS = 64
LANES = 128
ROWS_PER_TILE = LANES // BS
PLANE = BS * BS // LANES
NT = (((1,), (1,)), ((), ()))


def split3(x):
    hi = x.astype(jnp.bfloat16)
    rest = x - hi.astype(jnp.float32)
    mid = rest.astype(jnp.bfloat16)
    low = (rest - mid.astype(jnp.float32)).astype(jnp.bfloat16)
    return hi.astype(jnp.float32), mid.astype(jnp.float32), low.astype(jnp.float32)


def pack_kernel(
    bricks,
    capacity,
    owner_hbm,
    coords_hbm,
    fracs_hbm,
    request_ref,
    rank_ref,
    owner_ref,
    coords_ref,
    fracs_ref,
    sem,
):
    copies = [
        pltpu.make_async_copy(source, target, sem.at[c])
        for c, (source, target) in enumerate(
            ((owner_hbm, owner_ref), (coords_hbm, coords_ref), (fracs_hbm, fracs_ref))
        )
    ]
    for copy in copies:
        copy.start()
    for copy in copies:
        copy.wait()
    tracers = owner_ref.shape[1]
    groups = tracers // LANES
    owner = owner_ref[...]
    brick = lax.broadcasted_iota(jnp.int32, (bricks, LANES), 0)
    row = lax.broadcasted_iota(jnp.int32, (LANES, 2 * LANES), 0)
    column = lax.broadcasted_iota(jnp.int32, (LANES, 2 * LANES), 1)
    before = jnp.where((row < column) | (column >= LANES), 1.0, 0.0).astype(jnp.bfloat16)
    member = [
        jnp.where(owner[:, g * LANES : (g + 1) * LANES] == brick, 1.0, 0.0) for g in range(groups)
    ]
    counted = jnp.dot(
        jnp.concatenate(member, axis=0).astype(jnp.bfloat16),
        before,
        preferred_element_type=jnp.float32,
    )
    base = jnp.zeros((bricks, LANES), jnp.float32)
    ranks = []
    for g in range(groups):
        block = counted[g * bricks : (g + 1) * bricks]
        ranks.append(jnp.sum(member[g] * (block[:, :LANES] + base), axis=0, keepdims=True))
        base = base + block[:, LANES:]
    rank = jnp.concatenate(ranks, axis=1)
    rank_ref[...] = rank.astype(jnp.int32)
    place = lax.broadcasted_iota(jnp.int32, (LANES, tracers), 0) % capacity
    onehot = jnp.where(rank == place.astype(jnp.float32), 1.0, 0.0).astype(jnp.bfloat16)
    coords = coords_ref[...].astype(jnp.float32)
    hi, mid, low = split3(fracs_ref[...])
    one = jnp.zeros((1, tracers), jnp.float32)
    none = jnp.zeros((4, tracers), jnp.float32)
    parts = (
        jnp.concatenate([coords, one, hi, one], axis=0),
        jnp.concatenate([none, mid, one], axis=0),
        jnp.concatenate([none, low, one], axis=0),
    )
    total = None
    for part in parts:
        masked = jnp.concatenate(
            [jnp.where(owner == b, part, 0.0) for b in range(bricks)], axis=0
        ).astype(jnp.bfloat16)
        term = lax.dot_general(masked, onehot, NT, preferred_element_type=jnp.float32)
        total = term if total is None else total + term
    named = lax.broadcasted_iota(jnp.int32, (bricks, 8, LANES), 1) == 3
    request_ref[...] = jnp.where(named, base[:, None, :], total.reshape(bricks, 8, LANES))


def sample_kernel(
    bricks, capacity, request_ref, grid_ref, reply_ref, staged, where_ref, frac_ref, lines, sem
):
    blocks = 4 * capacity // LANES
    fractions = pltpu.make_async_copy(request_ref.at[:, 4, :], frac_ref, sem.at[0])
    fractions.start()
    asked = request_ref[...].astype(jnp.int32)
    second = jnp.concatenate([asked[:, 1:], asked[:, :1]], axis=1)
    shift = ROWS_PER_TILE.bit_length() - 1
    tile = asked * PLANE + (jnp.maximum(second - 1, 0) >> shift)
    turn = jnp.where(asked == 0, 0, jnp.where((asked & 1) == 1, BS, LANES))
    row = lax.broadcasted_iota(jnp.int32, asked.shape, 1)
    staged[...] = jnp.where(row == 0, tile, jnp.where(row == 1, turn, asked))
    copies = [
        pltpu.make_async_copy(staged.at[:, r, :], where_ref.at[c], sem.at[1 + c])
        for c, r in enumerate((0, 1, 3))
    ]
    for copy in copies:
        copy.start()
    lane = lax.broadcasted_iota(jnp.int32, (3, LANES), 1)
    fractions.wait()
    for copy in copies:
        copy.wait()
    chunk = 16

    def gather(p, carry):
        count = where_ref[2, p, 0]
        for c in range(0, capacity, chunk):

            @pl.when(count > c)
            def _():
                for r in range(c, c + chunk):
                    start = where_ref[0, p, r]
                    cut = lane < where_ref[1, p, r]
                    near = jnp.where(cut, grid_ref[start + 1], grid_ref[start])
                    far = jnp.where(cut, grid_ref[start + 1 + PLANE], grid_ref[start + PLANE])
                    line = near + frac_ref[p, r] * (far - near)
                    lines[pl.ds(p * (4 * capacity) + r, 3, stride=capacity), :] = line

        return carry

    lax.fori_loop(0, bricks, gather, 0)
    cell = lax.broadcasted_iota(jnp.int32, (BS, LANES), 0)

    def weigh(p):
        asked = request_ref[p]
        second = asked[1:2].astype(jnp.int32)
        third = asked[2:3].astype(jnp.int32)
        f1 = asked[5:6]
        f2 = asked[6:7]
        along = jnp.where(cell == third, 1.0 - f2, jnp.where(cell == third + 1, f2, 0.0))
        even = (second & 1) == 0
        top = jnp.where(even, 1.0 - f1, f1)
        bottom = jnp.where(even, f1, 1.0 - f1)
        rows = []
        for q in range(blocks):
            start = p * (4 * capacity) + q * LANES
            turned = lines[pl.ds(start, LANES), :].T
            crossed = turned[:BS] * top + turned[BS:] * bottom
            rows.append(jnp.sum(crossed * along, axis=0, keepdims=True))
        reply_ref[p] = jnp.concatenate(rows, axis=0)

    for p in range(bricks):
        weigh(p)


def advance_kernel(
    bricks,
    capacity,
    reply_ref,
    owner_ref,
    rank_ref,
    counts_ref,
    dist_ref,
    kernel_ref,
    redist_ref,
    shatter_ref,
    out_ref,
):
    tracers = owner_ref.shape[1]
    groups = tracers // LANES
    brick = lax.broadcasted_iota(jnp.int32, (bricks, LANES), 0)
    rows = [reply_ref[:, q, :] for q in range(reply_ref.shape[1])]
    fields = [[], [], []]
    for g in range(groups):
        lanes = slice(g * LANES, (g + 1) * LANES)
        mine = owner_ref[:, lanes] == brick
        rank = jnp.broadcast_to(rank_ref[:, lanes], (bricks, LANES))
        for f in range(3):
            q, offset = divmod(f * capacity, LANES)
            found = jnp.take_along_axis(rows[q], rank + offset, axis=1)
            fields[f].append(jnp.sum(jnp.where(mine, found, 0.0), axis=0, keepdims=True))
    density, temperature, metals = [jnp.concatenate(f, axis=1) for f in fields]
    coag = density * jnp.sqrt(temperature)
    shat = metals * temperature
    counts = counts_ref[...]
    h = 1.0 / jnp.maximum(counts, 1).astype(jnp.float32)

    def halves(x):
        hi = x.astype(jnp.bfloat16)
        return hi, (x - hi.astype(jnp.float32)).astype(jnp.bfloat16)

    def wide(x):
        hi, low = halves(x)
        return jnp.concatenate([hi, hi, low], axis=1)

    def tall(x):
        hi, low = halves(x)
        return jnp.concatenate([hi, low, hi], axis=0)

    def product(a, x):
        return jnp.dot(a, tall(x), preferred_element_type=jnp.float32)

    bins = dist_ref.shape[0]
    both = wide(jnp.concatenate([kernel_ref[...], shatter_ref[...]], axis=0))
    redist = wide(redist_ref[...])
    hcoag = h * coag
    hshat = h * shat
    n = dist_ref[...]
    for section in range(4):
        pair = product(both, n)
        kn = pair[:bins]
        broken = pair[bins:]
        moved = product(redist, n * kn)
        fresh = (n + (hcoag * moved + hshat * broken)) / (1.0 + (hcoag * kn + hshat))
        n = fresh if section == 0 else jnp.where(counts >= section + 1, fresh, n)
    out_ref[...] = n


def shards(grid, distribution, owner_ids, coords, fracs, counts, kernel, redist, shatter):
    bricks = lax.axis_size("brick")
    tracers = distribution.shape[1]
    capacity = 2 * tracers // bricks
    blocks = 4 * capacity // LANES
    owner = owner_ids.reshape(1, tracers)
    vmem = pl.BlockSpec(memory_space=pltpu.VMEM)
    request, rank = pl.pallas_call(
        functools.partial(pack_kernel, bricks, capacity),
        out_shape=(
            jax.ShapeDtypeStruct((bricks, 8, LANES), jnp.float32),
            jax.ShapeDtypeStruct((1, tracers), jnp.int32),
        ),
        in_specs=[pl.BlockSpec(memory_space=pltpu.HBM)] * 3,
        out_specs=(vmem, vmem),
        scratch_shapes=[
            pltpu.VMEM(owner.shape, owner.dtype),
            pltpu.VMEM(coords.shape, coords.dtype),
            pltpu.VMEM(fracs.shape, fracs.dtype),
            pltpu.SemaphoreType.DMA((3,)),
        ],
        cost_estimate=pl.CostEstimate(flops=20 << 30, bytes_accessed=1 << 20, transcendentals=0),
        compiler_params=pltpu.CompilerParams(vmem_limit_bytes=8 << 20),
        name="pack",
    )(*[pltpu.with_memory_space_constraint(x, pltpu.HBM) for x in (owner, coords, fracs)])
    asked = lax.all_to_all(request, "brick", split_axis=0, concat_axis=0, tiled=True)
    cells = grid.shape[1]
    tiles = grid.reshape(3, cells // LANES, LANES).transpose(1, 0, 2)
    reply = pl.pallas_call(
        functools.partial(sample_kernel, bricks, capacity),
        out_shape=jax.ShapeDtypeStruct((bricks, blocks, LANES), jnp.float32),
        in_specs=[vmem] * 2,
        out_specs=vmem,
        scratch_shapes=[
            pltpu.VMEM((bricks, 8, LANES), jnp.int32),
            pltpu.SMEM((3, bricks, LANES), jnp.int32),
            pltpu.SMEM((bricks, LANES), jnp.float32),
            pltpu.VMEM((bricks * 4 * capacity, LANES), jnp.float32),
            pltpu.SemaphoreType.DMA((4,)),
        ],
        compiler_params=pltpu.CompilerParams(vmem_limit_bytes=16 << 20),
        name="sample",
    )(asked, tiles)
    back = lax.all_to_all(reply, "brick", split_axis=0, concat_axis=0, tiled=True)
    return pl.pallas_call(
        functools.partial(advance_kernel, bricks, capacity),
        out_shape=jax.ShapeDtypeStruct(distribution.shape, jnp.float32),
        in_specs=[vmem] * 8,
        out_specs=vmem,
        compiler_params=pltpu.CompilerParams(vmem_limit_bytes=8 << 20),
        name="advance",
    )(back, owner, rank, counts.reshape(1, tracers), distribution, kernel, redist, shatter)


def solution(mesh):
    in_specs = (
        P(None, ("runs", "brick")),
        P(None, ("runs", "brick")),
        P(("runs", "brick"), None),
        P(None, ("runs", "brick")),
        P(None, ("runs", "brick")),
        P(("runs", "brick")),
        P(),
        P(),
        P(),
    )
    out_specs = P(None, ("runs", "brick"))
    return jax.shard_map(shards, mesh=mesh, in_specs=in_specs, out_specs=out_specs, check_vma=False)
```

```python
import functools

import jax
import jax.numpy as jnp
from jax import lax
from jax.experimental import pallas as pl
from jax.experimental.pallas import tpu as pltpu
from jax.sharding import PartitionSpec as P

BS = 64
LANES = 128
ROWS_PER_TILE = LANES // BS
PLANE = BS * BS // LANES
TURN = 1 << 24
NT = (((1,), (1,)), ((), ()))


def split3(x):
    hi = x.astype(jnp.bfloat16)
    rest = x - hi.astype(jnp.float32)
    mid = rest.astype(jnp.bfloat16)
    low = (rest - mid.astype(jnp.float32)).astype(jnp.bfloat16)
    return hi.astype(jnp.float32), mid.astype(jnp.float32), low.astype(jnp.float32)


def halves(x):
    hi = x.astype(jnp.bfloat16)
    return hi, (x - hi.astype(jnp.float32)).astype(jnp.bfloat16)


def wide(x):
    hi, low = halves(x)
    return jnp.concatenate([hi, hi, low], axis=1)


def product(a, x):
    hi, low = halves(x)
    tall = jnp.concatenate([hi, low, hi], axis=0)
    return jnp.dot(a, tall, preferred_element_type=jnp.float32)


def tables(kernel_ref, redist_ref, shatter_ref):
    both = jnp.concatenate([kernel_ref[...], shatter_ref[...]], axis=0)
    return wide(both), wide(redist_ref[...])


def collide(both, redist, n):
    pair = product(both, n)
    kn = pair[: n.shape[0]]
    return kn, pair[n.shape[0] :], product(redist, n * kn)


def pack_kernel(
    bricks,
    capacity,
    owner_hbm,
    coords_hbm,
    fracs_hbm,
    request_ref,
    rank_ref,
    owner_ref,
    coords_ref,
    fracs_ref,
    sem,
):
    copies = [
        pltpu.make_async_copy(source, target, sem.at[c])
        for c, (source, target) in enumerate(
            ((owner_hbm, owner_ref), (coords_hbm, coords_ref), (fracs_hbm, fracs_ref))
        )
    ]
    for copy in copies:
        copy.start()
    tracers = owner_ref.shape[1]
    groups = tracers // LANES
    brick = lax.broadcasted_iota(jnp.int32, (bricks, LANES), 0)
    row = lax.broadcasted_iota(jnp.int32, (LANES, 2 * LANES), 0)
    column = lax.broadcasted_iota(jnp.int32, (LANES, 2 * LANES), 1)
    before = jnp.where((row < column) | (column >= LANES), 1.0, 0.0).astype(jnp.bfloat16)
    place = lax.broadcasted_iota(jnp.int32, (LANES, tracers), 0) % capacity
    place = place.astype(jnp.float32)
    copies[0].wait()
    owner = owner_ref[...]
    member = [
        jnp.where(owner[:, g * LANES : (g + 1) * LANES] == brick, 1.0, 0.0) for g in range(groups)
    ]
    counted = jnp.dot(
        jnp.concatenate(member, axis=0).astype(jnp.bfloat16),
        before,
        preferred_element_type=jnp.float32,
    )
    base = jnp.zeros((bricks, LANES), jnp.float32)
    ranks = []
    for g in range(groups):
        block = counted[g * bricks : (g + 1) * bricks]
        ranks.append(jnp.sum(member[g] * (block[:, :LANES] + base), axis=0, keepdims=True))
        base = base + block[:, LANES:]
    rank = jnp.concatenate(ranks, axis=1)
    rank_ref[...] = rank.astype(jnp.int32)
    onehot = jnp.where(rank == place, 1.0, 0.0).astype(jnp.bfloat16)
    copies[1].wait()
    copies[2].wait()
    coords = coords_ref[...].astype(jnp.float32)
    hi, mid, low = split3(fracs_ref[...])
    one = jnp.zeros((1, tracers), jnp.float32)
    none = jnp.zeros((4, tracers), jnp.float32)
    parts = (
        jnp.concatenate([coords, one, hi, one], axis=0),
        jnp.concatenate([none, mid, one], axis=0),
        jnp.concatenate([none, low, one], axis=0),
    )
    total = None
    for part in parts:
        masked = jnp.concatenate(
            [jnp.where(owner == b, part, 0.0) for b in range(bricks)], axis=0
        ).astype(jnp.bfloat16)
        term = lax.dot_general(masked, onehot, NT, preferred_element_type=jnp.float32)
        total = term if total is None else total + term
    request_ref[...] = total.reshape(bricks, 8, LANES)


def sample_kernel(
    bricks,
    capacity,
    request_ref,
    grid_ref,
    dist_ref,
    kernel_ref,
    redist_ref,
    shatter_ref,
    reply_ref,
    first_ref,
    staged,
    code_ref,
    frac_ref,
    lines,
    sem,
):
    shift = ROWS_PER_TILE.bit_length() - 1
    step = 2
    spans = (pl.ds(0, step), pl.ds(step, bricks - step))
    early, late = copies = ([], [])

    def fetch(c, source, target):
        for k, span in enumerate(spans):
            copy = pltpu.make_async_copy(source(span), target.at[span], sem.at[k, c])
            copy.start()
            copies[k].append(copy)

    fetch(0, lambda span: request_ref.at[span, 4, :], frac_ref)
    asked = request_ref[...].astype(jnp.int32)
    second = jnp.concatenate([asked[:, 1:], asked[:, :1]], axis=1)
    tile = asked * PLANE + (jnp.maximum(second - 1, 0) >> shift)
    turn = jnp.where(second == 0, 0, jnp.where((second & 1) == 1, 1, 2))
    staged[...] = turn * TURN + tile
    fetch(1, lambda span: staged.at[span, 0, :], code_ref)
    side = jnp.where(lax.broadcasted_iota(jnp.int32, (3, LANES), 1) < BS, TURN, 2 * TURN)
    cell = lax.broadcasted_iota(jnp.int32, (BS, LANES), 0)
    pitch = capacity + 8
    height = 3 * pitch

    shared = 3 * capacity > LANES
    half = lax.broadcasted_iota(jnp.int32, (1, LANES), 1) < capacity

    def weights(p):
        asked = request_ref[p]
        second = asked[1:2].astype(jnp.int32)
        third = asked[2:3].astype(jnp.int32)
        f1 = asked[5:6]
        f2 = asked[6:7]
        along = jnp.where(cell == third, 1.0 - f2, jnp.where(cell == third + 1, f2, 0.0))
        even = (second & 1) == 0
        top = jnp.where(even, 1.0 - f1, f1)
        bottom = jnp.where(even, f1, 1.0 - f1)
        return top, bottom, along

    def weigh(pieces, factors):
        top, bottom, along = factors
        block = [lines[pl.ds(p * height + f * pitch, capacity), :] for p, f in pieces]
        used = len(block) * capacity
        turned = jnp.concatenate(block, axis=0).T
        crossed = turned[:BS] * top[:, :used] + turned[BS:] * bottom[:, :used]
        return jnp.sum(crossed * along[:, :used], axis=0, keepdims=True)

    def settle(p):
        factors = [weights(p + u) for u in range(step)]
        for u in range(step):
            fields = range(2 if shared else 3)
            total = weigh([(p + u, f) for f in fields], factors[u])
            reply_ref[p + u, 0:1, : total.shape[1]] = total
        if shared:
            mixed = [jnp.where(half, a, b) for a, b in zip(*factors)]
            total = weigh([(p + u, 2) for u in range(step)], mixed)
            for u in range(step):
                reply_ref[p + u, 1:2, :] = total

    bins = dist_ref.shape[0]
    both, redist = tables(kernel_ref, redist_ref, shatter_ref)
    for k, value in enumerate(collide(both, redist, dist_ref[...])):
        first_ref[k * bins : (k + 1) * bins] = value
    for copy in early:
        copy.wait()

    def gather(p):
        for r in range(capacity):
            code = code_ref[p, r]
            start = code & (TURN - 1)
            cut = code >= side
            near = jnp.where(cut, grid_ref[start + 1], grid_ref[start])
            far = jnp.where(cut, grid_ref[start + 1 + PLANE], grid_ref[start + PLANE])
            line = near + frac_ref[p, r] * (far - near)
            lines[pl.ds(p * height + r, 3, stride=pitch), :] = line

    def peers(q, carry):
        @pl.when(q == 1)
        def _():
            for copy in late:
                copy.wait()

        settle(jnp.maximum(step * (q - 1), 0))
        for u in range(step):
            gather(step * q + u)
        return carry

    lax.fori_loop(0, bricks // step, peers, 0)
    settle(bricks - step)


def advance_kernel(
    bricks,
    capacity,
    reply_ref,
    first_ref,
    owner_ref,
    rank_ref,
    counts_ref,
    dist_ref,
    kernel_ref,
    redist_ref,
    shatter_ref,
    out_ref,
):
    tracers = owner_ref.shape[1]
    groups = tracers // LANES
    brick = lax.broadcasted_iota(jnp.int32, (bricks, LANES), 0)
    rows = [reply_ref[:, q, :] for q in range(reply_ref.shape[1])]
    fields = [[], [], []]
    for g in range(groups):
        lanes = slice(g * LANES, (g + 1) * LANES)
        mine = owner_ref[:, lanes] == brick
        rank = jnp.broadcast_to(rank_ref[:, lanes], (bricks, LANES))
        for f in range(3):
            q, offset = divmod(f * capacity, LANES)
            if q:
                offset = capacity * (lax.axis_index("brick") % 2)
            found = jnp.take_along_axis(rows[q], rank + offset, axis=1)
            fields[f].append(jnp.sum(jnp.where(mine, found, 0.0), axis=0, keepdims=True))
    density, temperature, metals = [jnp.concatenate(f, axis=1) for f in fields]
    coag = density * jnp.sqrt(temperature)
    shat = metals * temperature
    counts = counts_ref[...]
    h = 1.0 / jnp.maximum(counts, 1).astype(jnp.float32)

    bins = dist_ref.shape[0]
    both, redist = tables(kernel_ref, redist_ref, shatter_ref)
    hcoag = h * coag
    hshat = h * shat
    n = dist_ref[...]
    for section in range(4):
        if section == 0:
            kn, broken, moved = (first_ref[k * bins : (k + 1) * bins] for k in range(3))
        else:
            kn, broken, moved = collide(both, redist, n)
        fresh = (n + (hcoag * moved + hshat * broken)) / (1.0 + (hcoag * kn + hshat))
        n = fresh if section == 0 else jnp.where(counts >= section + 1, fresh, n)
    out_ref[...] = n


def shards(grid, distribution, owner_ids, coords, fracs, counts, kernel, redist, shatter):
    bricks = lax.axis_size("brick")
    tracers = distribution.shape[1]
    capacity = 2 * tracers // bricks
    blocks = 4 * capacity // LANES
    owner = owner_ids.reshape(1, tracers)
    vmem = pl.BlockSpec(memory_space=pltpu.VMEM)
    request, rank = pl.pallas_call(
        functools.partial(pack_kernel, bricks, capacity),
        out_shape=(
            jax.ShapeDtypeStruct((bricks, 8, LANES), jnp.float32),
            jax.ShapeDtypeStruct((1, tracers), jnp.int32),
        ),
        in_specs=[pl.BlockSpec(memory_space=pltpu.HBM)] * 3,
        out_specs=(vmem, vmem),
        scratch_shapes=[
            pltpu.VMEM(owner.shape, owner.dtype),
            pltpu.VMEM(coords.shape, coords.dtype),
            pltpu.VMEM(fracs.shape, fracs.dtype),
            pltpu.SemaphoreType.DMA((3,)),
        ],
        cost_estimate=pl.CostEstimate(flops=20 << 30, bytes_accessed=1 << 20, transcendentals=0),
        compiler_params=pltpu.CompilerParams(vmem_limit_bytes=8 << 20),
        name="pack",
    )(*[pltpu.with_memory_space_constraint(x, pltpu.HBM) for x in (owner, coords, fracs)])
    asked = lax.all_to_all(request, "brick", split_axis=0, concat_axis=0, tiled=True)
    cells = grid.shape[1]
    tiles = grid.reshape(3, cells // LANES, LANES).transpose(1, 0, 2)
    reply, first = pl.pallas_call(
        functools.partial(sample_kernel, bricks, capacity),
        out_shape=(
            jax.ShapeDtypeStruct((bricks, blocks, LANES), jnp.float32),
            jax.ShapeDtypeStruct((3 * distribution.shape[0], tracers), jnp.float32),
        ),
        in_specs=[vmem] * 6,
        out_specs=(vmem, vmem),
        scratch_shapes=[
            pltpu.VMEM((bricks, 8, LANES), jnp.int32),
            pltpu.SMEM((bricks, LANES), jnp.int32),
            pltpu.SMEM((bricks, LANES), jnp.float32),
            pltpu.VMEM((bricks * 3 * (capacity + 8), LANES), jnp.float32),
            pltpu.SemaphoreType.DMA((2, 2)),
        ],
        compiler_params=pltpu.CompilerParams(vmem_limit_bytes=16 << 20),
        name="sample",
    )(asked, tiles, distribution, kernel, redist, shatter)
    back = lax.all_to_all(reply, "brick", split_axis=0, concat_axis=0, tiled=True)
    return pl.pallas_call(
        functools.partial(advance_kernel, bricks, capacity),
        out_shape=jax.ShapeDtypeStruct(distribution.shape, jnp.float32),
        in_specs=[vmem] * 9,
        out_specs=vmem,
        compiler_params=pltpu.CompilerParams(vmem_limit_bytes=8 << 20),
        name="advance",
    )(back, first, owner, rank, counts.reshape(1, tracers), distribution, kernel, redist, shatter)


def solution(mesh):
    in_specs = (
        P(None, ("runs", "brick")),
        P(None, ("runs", "brick")),
        P(("runs", "brick"), None),
        P(None, ("runs", "brick")),
        P(None, ("runs", "brick")),
        P(("runs", "brick")),
        P(),
        P(),
        P(),
    )
    out_specs = P(None, ("runs", "brick"))
    return jax.shard_map(shards, mesh=mesh, in_specs=in_specs, out_specs=out_specs, check_vma=False)
```

```python
import functools

import jax
import jax.numpy as jnp
from jax import lax
from jax.experimental import pallas as pl
from jax.experimental.pallas import tpu as pltpu
from jax.sharding import PartitionSpec as P

BS = 64
LANES = 128
HALF = LANES // 2
ROWS_PER_TILE = LANES // BS
PLANE = BS * BS // LANES
TURN = 1 << 24
NT = (((1,), (1,)), ((), ()))


def split3(x):
    hi = x.astype(jnp.bfloat16)
    rest = x - hi.astype(jnp.float32)
    mid = rest.astype(jnp.bfloat16)
    low = (rest - mid.astype(jnp.float32)).astype(jnp.bfloat16)
    return hi.astype(jnp.float32), mid.astype(jnp.float32), low.astype(jnp.float32)


def halves(x):
    hi = x.astype(jnp.bfloat16)
    return hi, (x - hi.astype(jnp.float32)).astype(jnp.bfloat16)


def wide(x):
    hi, low = halves(x)
    return jnp.concatenate([hi, hi, low], axis=1)


def product(a, x):
    hi, low = halves(x)
    tall = jnp.concatenate([hi, low, hi], axis=0)
    return jnp.dot(a, tall, preferred_element_type=jnp.float32)


def tables(kernel_ref, redist_ref, shatter_ref):
    both = jnp.concatenate([kernel_ref[...], shatter_ref[...]], axis=0)
    return wide(both), wide(redist_ref[...])


def collide(both, redist, n):
    pair = product(both, n)
    kn = pair[: n.shape[0]]
    return kn, pair[n.shape[0] :], product(redist, n * kn)


def pack_kernel(
    bricks,
    capacity,
    owner_hbm,
    coords_hbm,
    fracs_hbm,
    request_ref,
    rank_ref,
    owner_ref,
    coords_ref,
    fracs_ref,
    sem,
):
    copies = [
        pltpu.make_async_copy(source, target, sem.at[c])
        for c, (source, target) in enumerate(
            ((owner_hbm, owner_ref), (coords_hbm, coords_ref), (fracs_hbm, fracs_ref))
        )
    ]
    for copy in copies:
        copy.start()
    tracers = owner_ref.shape[1]
    groups = tracers // LANES
    brick = lax.broadcasted_iota(jnp.int32, (bricks, LANES), 0)
    row = lax.broadcasted_iota(jnp.int32, (LANES, 2 * LANES), 0)
    column = lax.broadcasted_iota(jnp.int32, (LANES, 2 * LANES), 1)
    before = jnp.where((row < column) | (column >= LANES), 1.0, 0.0).astype(jnp.bfloat16)
    lane = lax.broadcasted_iota(jnp.int32, (LANES, tracers), 0)
    place = (lane % capacity).astype(jnp.float32)
    left = lane < HALF
    nobody = jnp.full((LANES, tracers), -1.0, jnp.float32)
    places = (jnp.where(left, place, nobody), jnp.where(left, nobody, place))
    copies[0].wait()
    owner = owner_ref[...]
    member = [
        jnp.where(owner[:, g * LANES : (g + 1) * LANES] == brick, 1.0, 0.0) for g in range(groups)
    ]
    counted = jnp.dot(
        jnp.concatenate(member, axis=0).astype(jnp.bfloat16),
        before,
        preferred_element_type=jnp.float32,
    )
    base = jnp.zeros((bricks, LANES), jnp.float32)
    ranks = []
    for g in range(groups):
        block = counted[g * bricks : (g + 1) * bricks]
        ranks.append(jnp.sum(member[g] * (block[:, :LANES] + base), axis=0, keepdims=True))
        base = base + block[:, LANES:]
    rank = jnp.concatenate(ranks, axis=1)
    rank_ref[...] = rank.astype(jnp.int32)
    places = [jnp.where(rank == x, 1.0, 0.0).astype(jnp.bfloat16) for x in places]
    copies[1].wait()
    copies[2].wait()
    coords = coords_ref[...].astype(jnp.float32)
    hi, mid, low = split3(fracs_ref[...])
    none = jnp.zeros((3, tracers), jnp.float32)
    rows = bricks * 4
    mine = owner == lax.broadcasted_iota(jnp.int32, (rows, tracers), 0) // 4
    total = None
    for x in (hi, mid, low):
        first = coords if total is None else none
        for onehot, lines in ((0, (first, x[:1])), (1, (x[1:], none[:2]))):
            block = jnp.concatenate(lines, axis=0)
            pair = jnp.concatenate([block, block], axis=0)
            masked = jnp.concatenate([pair] * (bricks // 2), axis=0)
            masked = jnp.where(mine, masked, 0.0).astype(jnp.bfloat16)
            term = lax.dot_general(
                masked, places[onehot], NT, preferred_element_type=jnp.float32
            )
            total = term if total is None else total + term
    for b in range(bricks):
        request_ref[b] = total[4 * b : 4 * b + 4]


def sample_kernel(
    bricks,
    capacity,
    request_ref,
    grid_ref,
    dist_ref,
    kernel_ref,
    redist_ref,
    shatter_ref,
    reply_ref,
    first_ref,
    staged,
    code_ref,
    frac_ref,
    both_ref,
    lines,
    sem,
):
    shift = ROWS_PER_TILE.bit_length() - 1
    step = 2
    spans = (pl.ds(0, step), pl.ds(step, bricks - step))
    early, late = copies = ([], [])

    def fetch(c, source, target):
        for k, span in enumerate(spans):
            copy = pltpu.make_async_copy(source(span), target.at[span], sem.at[k, c])
            copy.start()
            copies[k].append(copy)

    fetch(0, lambda span: request_ref.at[span, 3, :], frac_ref)
    asked = request_ref[...].astype(jnp.int32)
    second = jnp.concatenate([asked[:, 1:], asked[:, :1]], axis=1)
    tile = asked * PLANE + (jnp.maximum(second - 1, 0) >> shift)
    turn = jnp.where(second == 0, 0, jnp.where((second & 1) == 1, 1, 2))
    staged[...] = turn * TURN + tile
    fetch(1, lambda span: staged.at[span, 0, :], code_ref)
    side = jnp.where(lax.broadcasted_iota(jnp.int32, (3, LANES), 1) < BS, TURN, 2 * TURN)
    cell = lax.broadcasted_iota(jnp.int32, (BS, LANES), 0).astype(jnp.float32)
    pitch = capacity + 8
    height = 3 * pitch

    shared = 3 * capacity > LANES
    half = lax.broadcasted_iota(jnp.int32, (1, LANES), 1) < capacity

    def weights(p):
        here = request_ref[p]
        turned = jnp.concatenate([here[:, HALF:], here[:, :HALF]], axis=1)
        asked = jnp.concatenate([jnp.where(former, here, turned), jnp.where(former, turned, here)], axis=0)
        second = asked[1:2].astype(jnp.int32)
        third = asked[2:3]
        f1 = asked[4:5]
        f2 = asked[5:6]
        along = jnp.where(cell == third, 1.0 - f2, jnp.where(cell == third + 1.0, f2, 0.0))
        even = (second & 1) == 0
        top = jnp.where(even, 1.0 - f1, f1)
        bottom = jnp.where(even, f1, 1.0 - f1)
        return top, bottom, along

    def weigh(pieces, factors):
        top, bottom, along = factors
        block = [lines[pl.ds(p * height + f * pitch, capacity), :] for p, f in pieces]
        used = len(block) * capacity
        turned = jnp.concatenate(block, axis=0).T
        crossed = turned[:BS] * top[:, :used] + turned[BS:] * bottom[:, :used]
        return jnp.sum(crossed * along[:, :used], axis=0, keepdims=True)

    def settle(p):
        factors = [weights(p + u) for u in range(step)]
        for u in range(step):
            fields = range(2 if shared else 3)
            total = weigh([(p + u, f) for f in fields], factors[u])
            reply_ref[p + u, 0:1, : total.shape[1]] = total
        if shared:
            mixed = [jnp.where(half, a, b) for a, b in zip(*factors)]
            total = weigh([(p + u, 2) for u in range(step)], mixed)
            for u in range(step):
                reply_ref[p + u, 1:2, :] = total

    former = lax.broadcasted_iota(jnp.int32, (4, LANES), 1) < HALF
    bins = dist_ref.shape[0]
    both, redist = tables(kernel_ref, redist_ref, shatter_ref)
    for k, value in enumerate(collide(both, redist, dist_ref[...])):
        first_ref[k * bins : (k + 1) * bins] = value
    for copy in early:
        copy.wait()

    def gather(p):
        for r in range(capacity):
            code = code_ref[p, r]
            start = code & (TURN - 1)
            cut = code >= side
            near = jnp.where(cut, grid_ref[start + 1], grid_ref[start])
            far = jnp.where(cut, grid_ref[start + 1 + PLANE], grid_ref[start + PLANE])
            line = near + frac_ref[p, r] * (far - near)
            lines[pl.ds(p * height + r, 3, stride=pitch), :] = line

    def peers(q, carry):
        @pl.when(q == 1)
        def _():
            for copy in late:
                copy.wait()

        settle(jnp.maximum(step * (q - 1), 0))
        for u in range(step):
            gather(step * q + u)
        return carry

    lax.fori_loop(0, bricks // step, peers, 0)
    settle(bricks - step)


def advance_kernel(
    bricks,
    capacity,
    reply_ref,
    first_ref,
    owner_ref,
    rank_ref,
    counts_ref,
    dist_ref,
    kernel_ref,
    redist_ref,
    shatter_ref,
    out_ref,
):
    tracers = owner_ref.shape[1]
    groups = tracers // LANES
    brick = lax.broadcasted_iota(jnp.int32, (bricks, LANES), 0)
    rows = [reply_ref[:, q, :] for q in range(reply_ref.shape[1])]
    fields = [[], [], []]
    for g in range(groups):
        lanes = slice(g * LANES, (g + 1) * LANES)
        mine = owner_ref[:, lanes] == brick
        rank = jnp.broadcast_to(rank_ref[:, lanes], (bricks, LANES))
        for f in range(3):
            q, offset = divmod(f * capacity, LANES)
            if q:
                offset = capacity * (lax.axis_index("brick") % 2)
            found = jnp.take_along_axis(rows[q], rank + offset, axis=1)
            fields[f].append(jnp.sum(jnp.where(mine, found, 0.0), axis=0, keepdims=True))
    density, temperature, metals = [jnp.concatenate(f, axis=1) for f in fields]
    coag = density * jnp.sqrt(temperature)
    shat = metals * temperature
    counts = counts_ref[...]
    h = 1.0 / jnp.maximum(counts, 1).astype(jnp.float32)

    bins = dist_ref.shape[0]
    both, redist = tables(kernel_ref, redist_ref, shatter_ref)
    hcoag = h * coag
    hshat = h * shat
    n = dist_ref[...]
    for section in range(4):
        if section == 0:
            kn, broken, moved = (first_ref[k * bins : (k + 1) * bins] for k in range(3))
        else:
            kn, broken, moved = collide(both, redist, n)
        fresh = (n + (hcoag * moved + hshat * broken)) / (1.0 + (hcoag * kn + hshat))
        n = fresh if section == 0 else jnp.where(counts >= section + 1, fresh, n)
    out_ref[...] = n


def shards(grid, distribution, owner_ids, coords, fracs, counts, kernel, redist, shatter):
    bricks = lax.axis_size("brick")
    tracers = distribution.shape[1]
    capacity = 2 * tracers // bricks
    blocks = 4 * capacity // LANES
    owner = owner_ids.reshape(1, tracers)
    vmem = pl.BlockSpec(memory_space=pltpu.VMEM)
    request, rank = pl.pallas_call(
        functools.partial(pack_kernel, bricks, capacity),
        out_shape=(
            jax.ShapeDtypeStruct((bricks, 4, LANES), jnp.float32),
            jax.ShapeDtypeStruct((1, tracers), jnp.int32),
        ),
        in_specs=[pl.BlockSpec(memory_space=pltpu.HBM)] * 3,
        out_specs=(vmem, vmem),
        scratch_shapes=[
            pltpu.VMEM(owner.shape, owner.dtype),
            pltpu.VMEM(coords.shape, coords.dtype),
            pltpu.VMEM(fracs.shape, fracs.dtype),
            pltpu.SemaphoreType.DMA((3,)),
        ],
        cost_estimate=pl.CostEstimate(flops=20 << 30, bytes_accessed=1 << 20, transcendentals=0),
        compiler_params=pltpu.CompilerParams(vmem_limit_bytes=8 << 20),
        name="pack",
    )(*[pltpu.with_memory_space_constraint(x, pltpu.HBM) for x in (owner, coords, fracs)])
    asked = lax.all_to_all(request, "brick", split_axis=0, concat_axis=0, tiled=True)
    cells = grid.shape[1]
    tiles = grid.reshape(3, cells // LANES, LANES).transpose(1, 0, 2)
    reply, first = pl.pallas_call(
        functools.partial(sample_kernel, bricks, capacity),
        out_shape=(
            jax.ShapeDtypeStruct((bricks, blocks, LANES), jnp.float32),
            jax.ShapeDtypeStruct((3 * distribution.shape[0], tracers), jnp.float32),
        ),
        in_specs=[vmem] * 6,
        out_specs=(vmem, vmem),
        scratch_shapes=[
            pltpu.VMEM((bricks, 4, LANES), jnp.int32),
            pltpu.SMEM((bricks, LANES), jnp.int32),
            pltpu.SMEM((bricks, LANES), jnp.float32),
            pltpu.VMEM((bricks, 8, LANES), jnp.float32),
            pltpu.VMEM((bricks * 3 * (capacity + 8), LANES), jnp.float32),
            pltpu.SemaphoreType.DMA((2, 2)),
        ],
        compiler_params=pltpu.CompilerParams(vmem_limit_bytes=16 << 20),
        name="sample",
    )(asked, tiles, distribution, kernel, redist, shatter)
    back = lax.all_to_all(reply, "brick", split_axis=0, concat_axis=0, tiled=True)
    return pl.pallas_call(
        functools.partial(advance_kernel, bricks, capacity),
        out_shape=jax.ShapeDtypeStruct(distribution.shape, jnp.float32),
        in_specs=[vmem] * 9,
        out_specs=vmem,
        compiler_params=pltpu.CompilerParams(vmem_limit_bytes=8 << 20),
        name="advance",
    )(back, first, owner, rank, counts.reshape(1, tracers), distribution, kernel, redist, shatter)


def solution(mesh):
    in_specs = (
        P(None, ("runs", "brick")),
        P(None, ("runs", "brick")),
        P(("runs", "brick"), None),
        P(None, ("runs", "brick")),
        P(None, ("runs", "brick")),
        P(("runs", "brick")),
        P(),
        P(),
        P(),
    )
    out_specs = P(None, ("runs", "brick"))
    return jax.shard_map(shards, mesh=mesh, in_specs=in_specs, out_specs=out_specs, check_vma=False)
```

```python
import functools

import jax
import jax.numpy as jnp
from jax import lax
from jax.experimental import pallas as pl
from jax.experimental.pallas import tpu as pltpu
from jax.sharding import PartitionSpec as P

BS = 64
LANES = 128
HALF = LANES // 2
ROWS_PER_TILE = LANES // BS
PLANE = BS * BS // LANES
TURN = 1 << 24
NT = (((1,), (1,)), ((), ()))


def split3(x):
    hi = x.astype(jnp.bfloat16)
    rest = x - hi.astype(jnp.float32)
    mid = rest.astype(jnp.bfloat16)
    low = (rest - mid.astype(jnp.float32)).astype(jnp.bfloat16)
    return hi.astype(jnp.float32), mid.astype(jnp.float32), low.astype(jnp.float32)


def halves(x):
    hi = x.astype(jnp.bfloat16)
    return hi, (x - hi.astype(jnp.float32)).astype(jnp.bfloat16)


def wide(x):
    hi, low = halves(x)
    return jnp.concatenate([hi, hi, low], axis=1)


def product(a, x):
    hi, low = halves(x)
    tall = jnp.concatenate([hi, low, hi], axis=0)
    return jnp.dot(a, tall, preferred_element_type=jnp.float32)


def tables(kernel_ref, redist_ref, shatter_ref):
    both = jnp.concatenate([kernel_ref[...], shatter_ref[...]], axis=0)
    return wide(both), wide(redist_ref[...])


def collide(both, redist, n):
    pair = product(both, n)
    kn = pair[: n.shape[0]]
    return kn, pair[n.shape[0] :], product(redist, n * kn)


def pack_kernel(
    bricks,
    capacity,
    owner_hbm,
    coords_hbm,
    fracs_hbm,
    request_ref,
    rank_ref,
    owner_ref,
    coords_ref,
    fracs_ref,
    sem,
):
    copies = [
        pltpu.make_async_copy(source, target, sem.at[c])
        for c, (source, target) in enumerate(
            ((owner_hbm, owner_ref), (coords_hbm, coords_ref), (fracs_hbm, fracs_ref))
        )
    ]
    for copy in copies:
        copy.start()
    tracers = owner_ref.shape[1]
    groups = tracers // LANES
    brick = lax.broadcasted_iota(jnp.int32, (bricks, LANES), 0)
    row = lax.broadcasted_iota(jnp.int32, (LANES, 2 * LANES), 0)
    column = lax.broadcasted_iota(jnp.int32, (LANES, 2 * LANES), 1)
    before = jnp.where((row < column) | (column >= LANES), 1.0, 0.0).astype(jnp.bfloat16)
    place = lax.broadcasted_iota(jnp.int32, (LANES, tracers), 0) % capacity
    place = place.astype(jnp.float32)
    copies[0].wait()
    owner = owner_ref[...]
    member = [
        jnp.where(owner[:, g * LANES : (g + 1) * LANES] == brick, 1.0, 0.0) for g in range(groups)
    ]
    counted = jnp.dot(
        jnp.concatenate(member, axis=0).astype(jnp.bfloat16),
        before,
        preferred_element_type=jnp.float32,
    )
    base = jnp.zeros((bricks, LANES), jnp.float32)
    ranks = []
    for g in range(groups):
        block = counted[g * bricks : (g + 1) * bricks]
        ranks.append(jnp.sum(member[g] * (block[:, :LANES] + base), axis=0, keepdims=True))
        base = base + block[:, LANES:]
    rank = jnp.concatenate(ranks, axis=1)
    rank_ref[...] = rank.astype(jnp.int32)
    onehot = jnp.where(rank == place, 1.0, 0.0).astype(jnp.bfloat16)
    copies[1].wait()
    copies[2].wait()
    coords = coords_ref[...].astype(jnp.float32)
    hi, mid, low = split3(fracs_ref[...])
    none = jnp.zeros((1, tracers), jnp.float32)
    rows = bricks * 4
    mine = owner == lax.broadcasted_iota(jnp.int32, (rows, tracers), 0) // 4

    def placed(*lines):
        block = jnp.concatenate(lines, axis=0)
        pair = jnp.concatenate([block, block], axis=0)
        masked = jnp.where(mine, jnp.concatenate([pair] * (bricks // 2), axis=0), 0.0)
        return lax.dot_general(
            masked.astype(jnp.bfloat16), onehot, NT, preferred_element_type=jnp.float32
        )

    cells = placed(coords, none)
    fractions = [placed(x[1:], none, x[:1]) for x in (hi, mid, low)]
    fractions = fractions[0] + fractions[1] + fractions[2]
    row = lax.broadcasted_iota(jnp.int32, (rows, LANES), 0) % 4
    lane = lax.broadcasted_iota(jnp.int32, (rows, LANES), 1)
    total = jnp.where((row < 3) & (lane < HALF), cells, fractions)
    for b in range(bricks):
        request_ref[b] = total[4 * b : 4 * b + 4]


def sample_kernel(
    bricks,
    capacity,
    request_ref,
    grid_ref,
    dist_ref,
    kernel_ref,
    redist_ref,
    shatter_ref,
    reply_ref,
    first_ref,
    staged,
    code_ref,
    frac_ref,
    both_ref,
    lines,
    sem,
):
    shift = ROWS_PER_TILE.bit_length() - 1
    step = 2
    spans = (pl.ds(0, step), pl.ds(step, bricks - step))
    early, late = copies = ([], [])

    def fetch(c, source, target):
        for k, span in enumerate(spans):
            copy = pltpu.make_async_copy(source(span), target.at[span], sem.at[k, c])
            copy.start()
            copies[k].append(copy)

    fetch(0, lambda span: request_ref.at[span, 3, :], frac_ref)
    asked = request_ref[...].astype(jnp.int32)
    second = jnp.concatenate([asked[:, 1:], asked[:, :1]], axis=1)
    tile = asked * PLANE + (jnp.maximum(second - 1, 0) >> shift)
    turn = jnp.where(second == 0, 0, jnp.where((second & 1) == 1, 1, 2))
    staged[...] = turn * TURN + tile
    fetch(1, lambda span: staged.at[span, 0, :], code_ref)
    side = jnp.where(lax.broadcasted_iota(jnp.int32, (3, LANES), 1) < BS, TURN, 2 * TURN)
    cell = lax.broadcasted_iota(jnp.int32, (BS, LANES), 0).astype(jnp.float32)
    pitch = capacity + 8
    height = 3 * pitch

    shared = 3 * capacity > LANES
    half = lax.broadcasted_iota(jnp.int32, (1, LANES), 1) < capacity

    def weights(p):
        here = request_ref[p]
        turned = jnp.concatenate([here[:, HALF:], here[:, :HALF]], axis=1)
        asked = jnp.concatenate([jnp.where(former, here, turned), jnp.where(former, turned, here)], axis=0)
        second = asked[1:2].astype(jnp.int32)
        third = asked[2:3]
        f1 = asked[4:5]
        f2 = asked[5:6]
        along = jnp.where(cell == third, 1.0 - f2, jnp.where(cell == third + 1.0, f2, 0.0))
        even = (second & 1) == 0
        top = jnp.where(even, 1.0 - f1, f1)
        bottom = jnp.where(even, f1, 1.0 - f1)
        return top, bottom, along

    def weigh(pieces, factors):
        top, bottom, along = factors
        block = [lines[pl.ds(p * height + f * pitch, capacity), :] for p, f in pieces]
        used = len(block) * capacity
        turned = jnp.concatenate(block, axis=0).T
        crossed = turned[:BS] * top[:, :used] + turned[BS:] * bottom[:, :used]
        return jnp.sum(crossed * along[:, :used], axis=0, keepdims=True)

    def settle(p):
        factors = [weights(p + u) for u in range(step)]
        for u in range(step):
            fields = range(2 if shared else 3)
            total = weigh([(p + u, f) for f in fields], factors[u])
            reply_ref[p + u, 0:1, : total.shape[1]] = total
        if shared:
            mixed = [jnp.where(half, a, b) for a, b in zip(*factors)]
            total = weigh([(p + u, 2) for u in range(step)], mixed)
            for u in range(step):
                reply_ref[p + u, 1:2, :] = total

    former = lax.broadcasted_iota(jnp.int32, (4, LANES), 1) < HALF
    bins = dist_ref.shape[0]
    both, redist = tables(kernel_ref, redist_ref, shatter_ref)
    for k, value in enumerate(collide(both, redist, dist_ref[...])):
        first_ref[k * bins : (k + 1) * bins] = value
    for copy in early:
        copy.wait()

    def gather(p):
        for r in range(capacity):
            code = code_ref[p, r]
            start = code & (TURN - 1)
            cut = code >= side
            near = jnp.where(cut, grid_ref[start + 1], grid_ref[start])
            far = jnp.where(cut, grid_ref[start + 1 + PLANE], grid_ref[start + PLANE])
            line = near + frac_ref[p, r] * (far - near)
            lines[pl.ds(p * height + r, 3, stride=pitch), :] = line

    def peers(q, carry):
        @pl.when(q == 1)
        def _():
            for copy in late:
                copy.wait()

        settle(jnp.maximum(step * (q - 1), 0))
        for u in range(step):
            gather(step * q + u)
        return carry

    lax.fori_loop(0, bricks // step, peers, 0)
    settle(bricks - step)


def advance_kernel(
    bricks,
    capacity,
    reply_ref,
    first_ref,
    owner_ref,
    rank_ref,
    counts_ref,
    dist_ref,
    kernel_ref,
    redist_ref,
    shatter_ref,
    out_ref,
):
    tracers = owner_ref.shape[1]
    groups = tracers // LANES
    brick = lax.broadcasted_iota(jnp.int32, (bricks, LANES), 0)
    rows = [reply_ref[:, q, :] for q in range(reply_ref.shape[1])]
    fields = [[], [], []]
    for g in range(groups):
        lanes = slice(g * LANES, (g + 1) * LANES)
        mine = owner_ref[:, lanes] == brick
        rank = jnp.broadcast_to(rank_ref[:, lanes], (bricks, LANES))
        for f in range(3):
            q, offset = divmod(f * capacity, LANES)
            if q:
                offset = capacity * (lax.axis_index("brick") % 2)
            found = jnp.take_along_axis(rows[q], rank + offset, axis=1)
            fields[f].append(jnp.sum(jnp.where(mine, found, 0.0), axis=0, keepdims=True))
    density, temperature, metals = [jnp.concatenate(f, axis=1) for f in fields]
    coag = density * jnp.sqrt(temperature)
    shat = metals * temperature
    counts = counts_ref[...]
    h = 1.0 / jnp.maximum(counts, 1).astype(jnp.float32)

    bins = dist_ref.shape[0]
    both, redist = tables(kernel_ref, redist_ref, shatter_ref)
    hcoag = h * coag
    hshat = h * shat
    n = dist_ref[...]
    for section in range(4):
        if section == 0:
            kn, broken, moved = (first_ref[k * bins : (k + 1) * bins] for k in range(3))
        else:
            kn, broken, moved = collide(both, redist, n)
        fresh = (n + (hcoag * moved + hshat * broken)) / (1.0 + (hcoag * kn + hshat))
        n = fresh if section == 0 else jnp.where(counts >= section + 1, fresh, n)
    out_ref[...] = n


def shards(grid, distribution, owner_ids, coords, fracs, counts, kernel, redist, shatter):
    bricks = lax.axis_size("brick")
    tracers = distribution.shape[1]
    capacity = 2 * tracers // bricks
    blocks = 4 * capacity // LANES
    owner = owner_ids.reshape(1, tracers)
    vmem = pl.BlockSpec(memory_space=pltpu.VMEM)
    request, rank = pl.pallas_call(
        functools.partial(pack_kernel, bricks, capacity),
        out_shape=(
            jax.ShapeDtypeStruct((bricks, 4, LANES), jnp.float32),
            jax.ShapeDtypeStruct((1, tracers), jnp.int32),
        ),
        in_specs=[pl.BlockSpec(memory_space=pltpu.HBM)] * 3,
        out_specs=(vmem, vmem),
        scratch_shapes=[
            pltpu.VMEM(owner.shape, owner.dtype),
            pltpu.VMEM(coords.shape, coords.dtype),
            pltpu.VMEM(fracs.shape, fracs.dtype),
            pltpu.SemaphoreType.DMA((3,)),
        ],
        cost_estimate=pl.CostEstimate(flops=20 << 30, bytes_accessed=1 << 20, transcendentals=0),
        compiler_params=pltpu.CompilerParams(vmem_limit_bytes=8 << 20),
        name="pack",
    )(*[pltpu.with_memory_space_constraint(x, pltpu.HBM) for x in (owner, coords, fracs)])
    asked = lax.all_to_all(request, "brick", split_axis=0, concat_axis=0, tiled=True)
    cells = grid.shape[1]
    tiles = grid.reshape(3, cells // LANES, LANES).transpose(1, 0, 2)
    reply, first = pl.pallas_call(
        functools.partial(sample_kernel, bricks, capacity),
        out_shape=(
            jax.ShapeDtypeStruct((bricks, blocks, LANES), jnp.float32),
            jax.ShapeDtypeStruct((3 * distribution.shape[0], tracers), jnp.float32),
        ),
        in_specs=[vmem] * 6,
        out_specs=(vmem, vmem),
        scratch_shapes=[
            pltpu.VMEM((bricks, 4, LANES), jnp.int32),
            pltpu.SMEM((bricks, LANES), jnp.int32),
            pltpu.SMEM((bricks, LANES), jnp.float32),
            pltpu.VMEM((bricks, 8, LANES), jnp.float32),
            pltpu.VMEM((bricks * 3 * (capacity + 8), LANES), jnp.float32),
            pltpu.SemaphoreType.DMA((2, 2)),
        ],
        compiler_params=pltpu.CompilerParams(vmem_limit_bytes=16 << 20),
        name="sample",
    )(asked, tiles, distribution, kernel, redist, shatter)
    back = lax.all_to_all(reply, "brick", split_axis=0, concat_axis=0, tiled=True)
    return pl.pallas_call(
        functools.partial(advance_kernel, bricks, capacity),
        out_shape=jax.ShapeDtypeStruct(distribution.shape, jnp.float32),
        in_specs=[vmem] * 9,
        out_specs=vmem,
        compiler_params=pltpu.CompilerParams(vmem_limit_bytes=8 << 20),
        name="advance",
    )(back, first, owner, rank, counts.reshape(1, tracers), distribution, kernel, redist, shatter)


def solution(mesh):
    in_specs = (
        P(None, ("runs", "brick")),
        P(None, ("runs", "brick")),
        P(("runs", "brick"), None),
        P(None, ("runs", "brick")),
        P(None, ("runs", "brick")),
        P(("runs", "brick")),
        P(),
        P(),
        P(),
    )
    out_specs = P(None, ("runs", "brick"))
    return jax.shard_map(shards, mesh=mesh, in_specs=in_specs, out_specs=out_specs, check_vma=False)
```

```python
import functools

import jax
import jax.numpy as jnp
from jax import lax
from jax.experimental import pallas as pl
from jax.experimental.pallas import tpu as pltpu
from jax.sharding import PartitionSpec as P

BS = 64
LANES = 128
HALF = LANES // 2
ROWS_PER_TILE = LANES // BS
PLANE = BS * BS // LANES
TURN = 1 << 24
NT = (((1,), (1,)), ((), ()))


def split3(x):
    hi = x.astype(jnp.bfloat16)
    rest = x - hi.astype(jnp.float32)
    mid = rest.astype(jnp.bfloat16)
    low = (rest - mid.astype(jnp.float32)).astype(jnp.bfloat16)
    return hi.astype(jnp.float32), mid.astype(jnp.float32), low.astype(jnp.float32)


def halves(x):
    hi = x.astype(jnp.bfloat16)
    return hi, (x - hi.astype(jnp.float32)).astype(jnp.bfloat16)


def wide(x):
    hi, low = halves(x)
    return jnp.concatenate([hi, hi, low], axis=1)


def product(a, x):
    hi, low = halves(x)
    tall = jnp.concatenate([hi, low, hi], axis=0)
    return jnp.dot(a, tall, preferred_element_type=jnp.float32)


def tables(kernel_ref, redist_ref, shatter_ref):
    both = jnp.concatenate([kernel_ref[...], shatter_ref[...]], axis=0)
    return wide(both), wide(redist_ref[...])


def collide(both, redist, n):
    pair = product(both, n)
    kn = pair[: n.shape[0]]
    return kn, pair[n.shape[0] :], product(redist, n * kn)


def pack_kernel(
    bricks,
    capacity,
    owner_hbm,
    coords_hbm,
    fracs_hbm,
    request_ref,
    rank_ref,
    owner_ref,
    coords_ref,
    fracs_ref,
    sem,
):
    copies = [
        pltpu.make_async_copy(source, target, sem.at[c])
        for c, (source, target) in enumerate(
            ((owner_hbm, owner_ref), (coords_hbm, coords_ref), (fracs_hbm, fracs_ref))
        )
    ]
    for copy in copies:
        copy.start()
    tracers = owner_ref.shape[1]
    groups = tracers // LANES
    brick = lax.broadcasted_iota(jnp.int32, (bricks, LANES), 0)
    row = lax.broadcasted_iota(jnp.int32, (LANES, 2 * LANES), 0)
    column = lax.broadcasted_iota(jnp.int32, (LANES, 2 * LANES), 1)
    before = jnp.where((row < column) | (column >= LANES), 1.0, 0.0).astype(jnp.bfloat16)
    lane = lax.broadcasted_iota(jnp.int32, (LANES, tracers), 0)
    place = (lane % capacity).astype(jnp.float32)
    left = lane < HALF
    nobody = jnp.full((LANES, tracers), -1.0, jnp.float32)
    places = (jnp.where(left, place, nobody), jnp.where(left, nobody, place))
    copies[0].wait()
    owner = owner_ref[...]
    member = [
        jnp.where(owner[:, g * LANES : (g + 1) * LANES] == brick, 1.0, 0.0) for g in range(groups)
    ]
    counted = jnp.dot(
        jnp.concatenate(member, axis=0).astype(jnp.bfloat16),
        before,
        preferred_element_type=jnp.float32,
    )
    base = jnp.zeros((bricks, LANES), jnp.float32)
    ranks = []
    for g in range(groups):
        block = counted[g * bricks : (g + 1) * bricks]
        ranks.append(jnp.sum(member[g] * (block[:, :LANES] + base), axis=0, keepdims=True))
        base = base + block[:, LANES:]
    rank = jnp.concatenate(ranks, axis=1)
    rank_ref[...] = rank.astype(jnp.int32)
    places = [jnp.where(rank == x, 1.0, 0.0).astype(jnp.bfloat16) for x in places]
    copies[1].wait()
    copies[2].wait()
    coords = coords_ref[...].astype(jnp.float32)
    hi, mid, low = split3(fracs_ref[...])
    none = jnp.zeros((3, tracers), jnp.float32)
    rows = bricks * 4
    mine = owner == lax.broadcasted_iota(jnp.int32, (rows, tracers), 0) // 4
    total = None
    for x in (hi, mid, low):
        first = coords if total is None else none
        for onehot, lines in ((0, (first, x[:1])), (1, (x[1:], none[:2]))):
            block = jnp.concatenate(lines, axis=0)
            pair = jnp.concatenate([block, block], axis=0)
            masked = jnp.concatenate([pair] * (bricks // 2), axis=0)
            masked = jnp.where(mine, masked, 0.0).astype(jnp.bfloat16)
            term = lax.dot_general(
                masked, places[onehot], NT, preferred_element_type=jnp.float32
            )
            total = term if total is None else total + term
    for b in range(bricks):
        request_ref[b] = total[4 * b : 4 * b + 4]


def sample_kernel(
    bricks,
    capacity,
    request_ref,
    grid_ref,
    dist_ref,
    kernel_ref,
    redist_ref,
    shatter_ref,
    reply_ref,
    first_ref,
    both_out,
    redist_out,
    staged,
    code_ref,
    frac_ref,
    both_ref,
    lines,
    sem,
):
    shift = ROWS_PER_TILE.bit_length() - 1
    step = 2
    spans = (pl.ds(0, step), pl.ds(step, bricks - step))
    early, late = copies = ([], [])

    def fetch(c, source, target):
        for k, span in enumerate(spans):
            copy = pltpu.make_async_copy(source(span), target.at[span], sem.at[k, c])
            copy.start()
            copies[k].append(copy)

    fetch(0, lambda span: request_ref.at[span, 3, :], frac_ref)
    asked = request_ref[...].astype(jnp.int32)
    second = jnp.concatenate([asked[:, 1:], asked[:, :1]], axis=1)
    tile = asked * PLANE + (jnp.maximum(second - 1, 0) >> shift)
    turn = jnp.where(second == 0, 0, jnp.where((second & 1) == 1, 1, 2))
    staged[...] = turn * TURN + tile
    fetch(1, lambda span: staged.at[span, 0, :], code_ref)
    side = jnp.where(lax.broadcasted_iota(jnp.int32, (3, LANES), 1) < BS, TURN, 2 * TURN)
    cell = lax.broadcasted_iota(jnp.int32, (BS, LANES), 0).astype(jnp.float32)
    pitch = capacity + 8
    height = 3 * pitch

    shared = 3 * capacity > LANES
    half = lax.broadcasted_iota(jnp.int32, (1, LANES), 1) < capacity

    def weights(p):
        here = request_ref[p]
        turned = jnp.concatenate([here[:, HALF:], here[:, :HALF]], axis=1)
        asked = jnp.concatenate([jnp.where(former, here, turned), jnp.where(former, turned, here)], axis=0)
        second = asked[1:2].astype(jnp.int32)
        third = asked[2:3]
        f1 = asked[4:5]
        f2 = asked[5:6]
        along = jnp.where(cell == third, 1.0 - f2, jnp.where(cell == third + 1.0, f2, 0.0))
        even = (second & 1) == 0
        top = jnp.where(even, 1.0 - f1, f1)
        bottom = jnp.where(even, f1, 1.0 - f1)
        return top, bottom, along

    def weigh(pieces, factors):
        top, bottom, along = factors
        block = [lines[pl.ds(p * height + f * pitch, capacity), :] for p, f in pieces]
        used = len(block) * capacity
        turned = jnp.concatenate(block, axis=0).T
        crossed = turned[:BS] * top[:, :used] + turned[BS:] * bottom[:, :used]
        return jnp.sum(crossed * along[:, :used], axis=0, keepdims=True)

    def settle(p):
        factors = [weights(p + u) for u in range(step)]
        for u in range(step):
            fields = range(2 if shared else 3)
            total = weigh([(p + u, f) for f in fields], factors[u])
            reply_ref[p + u, 0:1, : total.shape[1]] = total
        if shared:
            mixed = [jnp.where(half, a, b) for a, b in zip(*factors)]
            total = weigh([(p + u, 2) for u in range(step)], mixed)
            for u in range(step):
                reply_ref[p + u, 1:2, :] = total

    former = lax.broadcasted_iota(jnp.int32, (4, LANES), 1) < HALF
    bins = dist_ref.shape[0]
    both, redist = tables(kernel_ref, redist_ref, shatter_ref)
    both_out[...] = both
    redist_out[...] = redist
    for k, value in enumerate(collide(both, redist, dist_ref[...])):
        first_ref[k * bins : (k + 1) * bins] = value
    for copy in early:
        copy.wait()

    def gather(p):
        for r in range(capacity):
            code = code_ref[p, r]
            start = code & (TURN - 1)
            cut = code >= side
            near = jnp.where(cut, grid_ref[start + 1], grid_ref[start])
            far = jnp.where(cut, grid_ref[start + 1 + PLANE], grid_ref[start + PLANE])
            line = near + frac_ref[p, r] * (far - near)
            lines[pl.ds(p * height + r, 3, stride=pitch), :] = line

    def peers(q, carry):
        @pl.when(q == 1)
        def _():
            for copy in late:
                copy.wait()

        settle(jnp.maximum(step * (q - 1), 0))
        for u in range(step):
            gather(step * q + u)
        return carry

    lax.fori_loop(0, bricks // step, peers, 0)
    settle(bricks - step)


def advance_kernel(
    bricks,
    capacity,
    reply_ref,
    first_ref,
    owner_ref,
    rank_ref,
    counts_ref,
    dist_ref,
    both_ref,
    redist_ref,
    out_ref,
):
    tracers = owner_ref.shape[1]
    groups = tracers // LANES
    brick = lax.broadcasted_iota(jnp.int32, (bricks, LANES), 0)
    rows = [reply_ref[:, q, :] for q in range(reply_ref.shape[1])]
    fields = [[], [], []]
    for g in range(groups):
        lanes = slice(g * LANES, (g + 1) * LANES)
        mine = owner_ref[:, lanes] == brick
        rank = jnp.broadcast_to(rank_ref[:, lanes], (bricks, LANES))
        for f in range(3):
            q, offset = divmod(f * capacity, LANES)
            if q:
                offset = capacity * (lax.axis_index("brick") % 2)
            found = jnp.take_along_axis(rows[q], rank + offset, axis=1)
            fields[f].append(jnp.sum(jnp.where(mine, found, 0.0), axis=0, keepdims=True))
    density, temperature, metals = [jnp.concatenate(f, axis=1) for f in fields]
    coag = density * jnp.sqrt(temperature)
    shat = metals * temperature
    counts = counts_ref[...]
    h = 1.0 / jnp.maximum(counts, 1).astype(jnp.float32)

    bins = dist_ref.shape[0]
    both, redist = both_ref[...], redist_ref[...]
    hcoag = h * coag
    hshat = h * shat
    n = dist_ref[...]
    for section in range(4):
        if section == 0:
            kn, broken, moved = (first_ref[k * bins : (k + 1) * bins] for k in range(3))
        else:
            kn, broken, moved = collide(both, redist, n)
        fresh = (n + (hcoag * moved + hshat * broken)) / (1.0 + (hcoag * kn + hshat))
        n = fresh if section == 0 else jnp.where(counts >= section + 1, fresh, n)
    out_ref[...] = n


def shards(grid, distribution, owner_ids, coords, fracs, counts, kernel, redist, shatter):
    bricks = lax.axis_size("brick")
    tracers = distribution.shape[1]
    capacity = 2 * tracers // bricks
    blocks = 4 * capacity // LANES
    owner = owner_ids.reshape(1, tracers)
    vmem = pl.BlockSpec(memory_space=pltpu.VMEM)
    request, rank = pl.pallas_call(
        functools.partial(pack_kernel, bricks, capacity),
        out_shape=(
            jax.ShapeDtypeStruct((bricks, 4, LANES), jnp.float32),
            jax.ShapeDtypeStruct((1, tracers), jnp.int32),
        ),
        in_specs=[pl.BlockSpec(memory_space=pltpu.HBM)] * 3,
        out_specs=(vmem, vmem),
        scratch_shapes=[
            pltpu.VMEM(owner.shape, owner.dtype),
            pltpu.VMEM(coords.shape, coords.dtype),
            pltpu.VMEM(fracs.shape, fracs.dtype),
            pltpu.SemaphoreType.DMA((3,)),
        ],
        cost_estimate=pl.CostEstimate(flops=20 << 30, bytes_accessed=1 << 20, transcendentals=0),
        compiler_params=pltpu.CompilerParams(vmem_limit_bytes=8 << 20),
        name="pack",
    )(*[pltpu.with_memory_space_constraint(x, pltpu.HBM) for x in (owner, coords, fracs)])
    asked = lax.all_to_all(request, "brick", split_axis=0, concat_axis=0, tiled=True)
    cells = grid.shape[1]
    tiles = grid.reshape(3, cells // LANES, LANES).transpose(1, 0, 2)
    bins = distribution.shape[0]
    reply, first, both, moving = pl.pallas_call(
        functools.partial(sample_kernel, bricks, capacity),
        out_shape=(
            jax.ShapeDtypeStruct((bricks, blocks, LANES), jnp.float32),
            jax.ShapeDtypeStruct((3 * bins, tracers), jnp.float32),
            jax.ShapeDtypeStruct((2 * bins, 3 * bins), jnp.bfloat16),
            jax.ShapeDtypeStruct((bins, 3 * bins), jnp.bfloat16),
        ),
        in_specs=[vmem] * 6,
        out_specs=(vmem,) * 4,
        scratch_shapes=[
            pltpu.VMEM((bricks, 4, LANES), jnp.int32),
            pltpu.SMEM((bricks, LANES), jnp.int32),
            pltpu.SMEM((bricks, LANES), jnp.float32),
            pltpu.VMEM((bricks, 8, LANES), jnp.float32),
            pltpu.VMEM((bricks * 3 * (capacity + 8), LANES), jnp.float32),
            pltpu.SemaphoreType.DMA((2, 2)),
        ],
        compiler_params=pltpu.CompilerParams(vmem_limit_bytes=16 << 20),
        name="sample",
    )(asked, tiles, distribution, kernel, redist, shatter)
    back = lax.all_to_all(reply, "brick", split_axis=0, concat_axis=0, tiled=True)
    return pl.pallas_call(
        functools.partial(advance_kernel, bricks, capacity),
        out_shape=jax.ShapeDtypeStruct(distribution.shape, jnp.float32),
        in_specs=[vmem] * 8,
        out_specs=vmem,
        compiler_params=pltpu.CompilerParams(vmem_limit_bytes=8 << 20),
        name="advance",
    )(back, first, owner, rank, counts.reshape(1, tracers), distribution, both, moving)


def solution(mesh):
    in_specs = (
        P(None, ("runs", "brick")),
        P(None, ("runs", "brick")),
        P(("runs", "brick"), None),
        P(None, ("runs", "brick")),
        P(None, ("runs", "brick")),
        P(("runs", "brick")),
        P(),
        P(),
        P(),
    )
    out_specs = P(None, ("runs", "brick"))
    return jax.shard_map(shards, mesh=mesh, in_specs=in_specs, out_specs=out_specs, check_vma=False)
```
